128 devices in a mesh: shot: 16 (over y, z), rcv: 8 (over x, core).
Axes of the slice: x: 4, y: 4, z: 4, core: 2. Of those that a mesh axis runs over, the one named last changes fastest.
Arguments:
- shot_data: bfloat16 [512, 2048, 256], P('shot', 'rcv'), may hold values from -0.25 to 0.25
- code: int32 [32, 512], P(None, 'shot'), may hold values from -1 to 1, as said below
- observed: bfloat16 [32, 2048, 256], P('shot', 'rcv'), may hold values from -6 to 6
- block_of: int32 [2048, 1], replicated, may hold values from 0 to 7; in each aligned block of 256 rows (0 to 255, 256 to 511, ...) at most 64 rows name the same one
- stencil_index: int32 [2048, 4], replicated, may hold values from 0 to 255
- stencil_weight: float32 [2048, 4], replicated, may hold values from -0.5 to 1
Outputs:
- adjoint_source: float32 [32, 2048, 256], P('shot', 'rcv')
The draws below stay inside these ranges and needn't reach their ends.
Inputs may be any that keep to these rules, and one draw needn't show every extreme that they name: `code`: every entry is -1 or 1. `block_of`: among the receivers of one index of rcv (aligned blocks of 256 rows) at most 64 map to one model block.
All inputs are finite; a program needn't handle non-finite values.
Results may differ from the reference program's by a relative error of at most 0.0038.
Values may be sent and summed in bfloat16 or wider, within the bound.
A program may use at most 64 MiB of HBM per device.

```python
import math
import jax
import jax.numpy as jnp
import numpy as np
from jax import lax

SUPERS = 32
RCV_DEV = 256
SAMPLES = 256
GRID = 256
STENCIL = 4
CAP = 64
SHOTS = 512
RECEIVERS = 2048
BLOCKS = 8


def draw_code(key, part):
    return (2 * jax.random.randint(key, (SUPERS, SHOTS), 0, 2) - 1).astype(jnp.int32)


def plant(array, own_key, least, largest):
    dims = array.shape
    index_at = [jax.random.randint(jax.random.fold_in(own_key, axis), (), 0, dims[axis]) for axis in range(len(dims))]
    array = array.at[tuple(index_at)].set(least)
    longest = dims.index(max(dims))
    index_at[longest] = (index_at[longest] + 1) % dims[longest]
    return array.at[tuple(index_at)].set(largest)


def level_of(rng, shape, shards, smallest, high):
    loudness = 1.0
    for axis_at, shards_of in shards:
        draws = jax.random.uniform(jax.random.fold_in(jax.random.fold_in(rng, 6), axis_at), (shards_of,), jnp.float32, smallest / len(shards), high / len(shards))
        loudness = loudness * jnp.repeat(jnp.exp(draws), shape[axis_at] // shards_of).reshape((-1,) + (1,) * (len(shape) - 1 - axis_at))
    return loudness


def deal_out(rng, own, number, rows, number_of, top, bound, skew):
    order = jax.random.permutation(rng, number_of)
    packed, common = shares(number_of, rows * top, bound, skew, True), shares(number_of, rows * top, bound, skew, False)
    places = jnp.arange(number_of)

    def named(lengths, rotation):
        used = int((lengths > 0).sum())
        fixed = max(1, used // 4)
        shifted = fixed + (places - fixed + rotation * (used - fixed)) % max(1, number_of - fixed)
        return jnp.zeros((number_of,), jnp.int32).at[order[jnp.where(places < fixed, places, shifted)]].set(jnp.asarray(lengths, jnp.int32))

    lengths = jnp.where(number % 4 == 0, named(packed, number // 4), named(common, number - number // 4 - 1))
    mixed = jax.random.permutation(jax.random.fold_in(own, 3), number_of)
    giver, taker = mixed[0:number_of // 2 * 2:2], mixed[1:number_of // 2 * 2:2]
    room = jnp.minimum(lengths[giver] - 1, bound - lengths[taker]) // 2
    room = jnp.where((giver == order[0]) | (taker == order[0]) | (lengths[taker] == 0), 0, jnp.maximum(room, 0))
    shifted = jax.random.randint(jax.random.fold_in(own, 4), (number_of // 2,), 0, 1 << 20) % (room + 1)
    lengths = lengths.at[giver].add(-shifted).at[taker].add(shifted)
    items = jnp.searchsorted(jnp.cumsum(lengths), jnp.arange(rows * top), side="right").astype(jnp.int32)
    listing = items.reshape(top, rows).T
    listing = listing[jax.random.permutation(jax.random.fold_in(own, 1), rows)]
    rotation = jax.random.randint(jax.random.fold_in(own, 2), (rows, 1), 0, top)
    return jnp.take_along_axis(listing, (jnp.arange(top)[None, :] + rotation) % top, axis=1)


def shares(number_of, total, bound, skew, full):
    weights = [(1 << 20) // math.isqrt(rank ** skew) + 1 for rank in range(1, number_of + 1)]
    largest = bound if full else min(bound, max(-(-total // number_of), total * weights[0] // sum(weights)))
    least = 1 if total - largest >= number_of - 1 else 0
    given, spare = [largest] + [least] * (number_of - 1), total - largest - least * (number_of - 1)
    while spare > 0:
        candidates = [i for i in range(1, number_of) if given[i] < largest] or [i for i in range(1, number_of) if given[i] < bound]
        mass, remaining = sum([weights[i] for i in candidates]), spare
        for i in candidates:
            addition = min(bound - given[i], max(1, remaining * weights[i] // mass), spare)
            given[i] = given[i] + addition
            spare = spare - addition
    return np.array(given)


def noise(key, extent, scale, reach, cuts=(), kind=jnp.bfloat16):
    values = jax.random.normal(key, extent, jnp.float32) * scale
    if len(cuts) > 0:
        values = level_of(key, extent, cuts, -0.22, 0.18) * values
    return jnp.clip(values, min=-reach, max=reach).astype(kind)


def setup_inputs(seed: int = 0) -> dict:
    seeds = jax.random.split(jax.random.key(seed), 7)
    shot_data = noise(seeds[0], (SHOTS, RECEIVERS, SAMPLES), SHOTS ** -0.5, 0.25, ((0, 16), (1, 8)))
    code = draw_code(jax.random.fold_in(seeds[6], 71), 0)
    observed = noise(seeds[2], (SUPERS, RECEIVERS, SAMPLES), 1.0, 6.0, ((0, 16), (1, 8)))
    block_of_keys = jax.random.split(jax.random.fold_in(seeds[3], 1), RECEIVERS // RCV_DEV)
    block_of_turns = jax.random.permutation(jax.random.fold_in(seeds[3], 3), RECEIVERS // RCV_DEV)
    block_of = jax.vmap(lambda own, number: deal_out(jax.random.fold_in(seeds[3], 2), own, number, RCV_DEV, BLOCKS, 1, CAP, 2))(block_of_keys, block_of_turns).reshape((RECEIVERS, 1))
    stencil_index = plant(jax.random.randint(seeds[4], (RECEIVERS, STENCIL), 0, GRID), jax.random.fold_in(seeds[4], 1), 0, GRID - 1).astype(jnp.int32)
    stencil_weight = jnp.clip(jax.random.uniform(seeds[5], (RECEIVERS, STENCIL), jnp.float32, -0.5, 1.0), -0.5, 1.0)
    return {"shot_data": shot_data, "code": code, "observed": observed, "block_of": block_of, "stencil_index": stencil_index, "stencil_weight": stencil_weight}


def spread_weights(stencil_index, stencil_weight):
    receivers = stencil_index.shape[0]
    points = jnp.arange(GRID, dtype=jnp.int32)[:, None]
    spread = jnp.zeros((GRID, receivers), jnp.float32)
    for which in range(STENCIL):
        spread = spread + jnp.where(points == stencil_index[:, which][None, :], stencil_weight[:, which][None, :], 0.0)
    return spread


def reference(shot_data, code, observed, block_of, stencil_index, stencil_weight):
    shots, receivers, samples = shot_data.shape
    flat_rows = shot_data.reshape(shots, receivers * samples)
    supershot = jnp.dot(code.astype(jnp.bfloat16), flat_rows, preferred_element_type=jnp.float32)
    supershot = supershot.reshape(SUPERS, receivers, samples)
    residual = (supershot - observed.astype(jnp.float32)).astype(jnp.bfloat16)
    spread = spread_weights(stencil_index, stencil_weight)
    block_ids = jnp.arange(BLOCKS, dtype=jnp.int32)[:, None, None]
    injection = jnp.where(block_ids == block_of[:, 0][None, None, :], spread[None], 0.0)
    injection = injection.reshape(BLOCKS * GRID, receivers).astype(jnp.bfloat16)
    return jnp.einsum("cr,krt->kct", injection.astype(jnp.float32), residual.astype(jnp.float32), precision=lax.Precision.HIGHEST)
```

```python
import jax
import jax.numpy as jnp
from jax import lax
from jax.experimental import pallas as pl
from jax.experimental.pallas import tpu as pltpu
from jax.sharding import PartitionSpec as P

SUPERS = 32
GRID = 256
STENCIL = 4
BLOCKS = 8
CAP = 64
RING = 4
RCV = 256
HALF = RCV // 2
SAMPLES = 256
LANES = 128
SHOTS_DEV = 32
GROUP = 16
ROWS = SUPERS * GROUP
DEPTH = SHOTS_DEV * GROUP
ORDER = (2, 1, 3, 0)
F32, BF16, I32 = jnp.float32, jnp.bfloat16, jnp.int32
MESH = pl.DeviceIdType.MESH


def iota(shape, dim):
    return lax.broadcasted_iota(I32, shape, dim)


def encoding_rows(shape, y, z):
    row = iota(shape, 0)
    kk = row // (ROWS // 2)
    first = (row // (4 * GROUP)) % 4
    spot = (row // GROUP) % 4
    second = jnp.where(spot == 0, 2, jnp.where(spot == 1, 1, jnp.where(spot == 2, 3, 0)))
    dy = jnp.where(kk == 0, first, second)
    dz = jnp.where(kk == 0, second, first)
    return 8 * ((y + dy) % 4) + 2 * ((z + dz) % 4) + kk


def kernel(
    shot_hbm, code_hbm, obs_hbm, blk_hbm, idx_hbm, wgt_hbm, out_hbm,
    xbuf, codebuf, obsbuf, blk, idx, wgt, enc, inj, injc, sel, obuf,
    own, keep, send1, recv1, send2, recv2, send3, recv3,
    load_sem, out_sem, s1_sem, r1_sem, s2_sem, r2_sem, s3_sem, r3_sem,
):
    shot, rcv = lax.axis_index("shot"), lax.axis_index("rcv")
    y, z = shot // 4, shot % 4

    def at_shot(dy, dz):
        return (((y + dy) % 4) * 4 + (z + dz) % 4, rcv)

    def neighbour(kk, stage, direction):
        step = 1 if direction == 0 else 3
        along_y = (kk == 0) == (stage == 1)
        return at_shot(step, 0) if along_y else at_shot(0, step)

    loads = [pltpu.make_async_copy(code_hbm, codebuf, load_sem.at[0])]
    for chunk in range(4):
        rows = pl.ds(chunk * 64, 64)
        loads.append(pltpu.make_async_copy(shot_hbm.at[:, rows], xbuf.at[:, rows], load_sem.at[1 + chunk]))
    loads.append(pltpu.make_async_copy(obs_hbm, obsbuf, load_sem.at[5]))
    loads.append(pltpu.make_async_copy(blk_hbm, blk, load_sem.at[6]))
    loads.append(pltpu.make_async_copy(idx_hbm, idx, load_sem.at[7]))
    loads.append(pltpu.make_async_copy(wgt_hbm, wgt, load_sem.at[8]))
    for load in loads:
        load.start()

    barrier = pltpu.get_barrier_semaphore()
    for peer in (at_shot(1, 0), at_shot(3, 0), at_shot(0, 1), at_shot(0, 3)):
        pl.semaphore_signal(barrier, inc=1, device_id=peer, device_id_type=MESH)
    for off in range(1, BLOCKS):
        pl.semaphore_signal(barrier, inc=1, device_id=(shot, (rcv + off) % BLOCKS), device_id_type=MESH)

    loads[0].wait()
    pick = (encoding_rows((ROWS, SUPERS), y, z) == iota((ROWS, SUPERS), 1)).astype(BF16)
    codes = jnp.dot(pick, codebuf[...].astype(F32).astype(BF16), preferred_element_type=F32).astype(BF16)
    widen = (iota((SHOTS_DEV, DEPTH), 1) // GROUP == iota((SHOTS_DEV, DEPTH), 0)).astype(BF16)
    wide = jnp.dot(codes, widen, preferred_element_type=F32)
    same = iota((ROWS, DEPTH), 0) % GROUP == iota((ROWS, DEPTH), 1) % GROUP
    enc[...] = jnp.where(same, wide, 0.0).astype(BF16)

    def half_rows(half):
        return pl.ds(half * HALF, HALF)

    def encode(half, chunk):
        def body(step, carry):
            r0 = pl.multiple_of(chunk * 64 + step * GROUP, GROUP)
            data = xbuf[:, pl.ds(r0, GROUP), :].reshape(DEPTH, SAMPLES)
            for kk in range(2):
                product = jnp.dot(enc[kk * 256:(kk + 1) * 256, :], data, preferred_element_type=F32)
                product = product.reshape(4, 4, GROUP, SAMPLES)
                for th in range(2):
                    part = product[:, :, :, th * LANES:(th + 1) * LANES]
                    rows = pl.ds(r0, GROUP)
                    inner = pl.ds(pl.multiple_of(r0 - half * HALF, GROUP), GROUP)
                    own[kk, th, :, rows, :] = part[0]
                    send1[kk, th, 1, :, rows, :] = part[2].astype(BF16)
                    if half == 0:
                        keep[kk, th, 0, :, inner, :] = part[1]
                        send1[kk, th, 2, :, rows, :] = part[3].astype(BF16)
                    else:
                        send1[kk, th, 0, :, rows, :] = part[1].astype(BF16)
                        keep[kk, th, 1, :, inner, :] = part[3]
            return carry

        lax.fori_loop(0, 4, body, 0)

    def copy1(kk, th, kind, direction, spot):
        slot = 1 if kind == 0 else (0 if direction == 0 else 2)
        half = direction if kind in (0, 2) else 1 - direction
        return pltpu.make_async_remote_copy(
            src_ref=send1.at[kk, th, slot, spot, half_rows(half)],
            dst_ref=recv1.at[kk, th, kind, direction, spot],
            send_sem=s1_sem.at[kk, th, kind, direction, spot],
            recv_sem=r1_sem.at[kk, th, kind, direction, spot],
            device_id=neighbour(kk, 1, direction),
            device_id_type=MESH,
        )

    def copy2(kk, th, kind, direction):
        slot = 1 if kind == 0 else (0 if direction == 0 else 2)
        half = direction if kind in (0, 2) else 1 - direction
        return pltpu.make_async_remote_copy(
            src_ref=send2.at[kk, th, slot, half_rows(half)],
            dst_ref=recv2.at[kk, th, kind, direction],
            send_sem=s2_sem.at[kk, th, kind, direction],
            recv_sem=r2_sem.at[kk, th, kind, direction],
            device_id=neighbour(kk, 2, direction),
            device_id_type=MESH,
        )

    def copy3(kk, th, off):
        block = (rcv + off) % BLOCKS
        return pltpu.make_async_remote_copy(
            src_ref=send3.at[kk, th, pl.ds(pl.multiple_of(block * CAP, CAP), CAP)],
            dst_ref=recv3.at[kk, th, pl.ds(pl.multiple_of(rcv * CAP, CAP), CAP)],
            send_sem=s3_sem.at[kk, th, off - 1],
            recv_sem=r3_sem.at[kk, th, off - 1],
            device_id=(shot, block),
            device_id_type=MESH,
        )

    pairs = [(kk, direction) for kk in range(2) for direction in range(2)]

    def start1(th, kind, spots, directions=(0, 1)):
        for spot in spots:
            for kk in range(2):
                for direction in directions:
                    copy1(kk, th, kind, direction, spot).start()

    def accumulate1(th, spot):
        for kk, direction in pairs:
            copy1(kk, th, 0, direction, spot).wait_recv()
            total = keep[kk, th, direction, spot] + recv1[kk, th, 0, direction, spot].astype(F32)
            send1[kk, th, 0 if direction == 0 else 2, spot, half_rows(direction), :] = total.astype(BF16)
            copy1(kk, th, 2, direction, spot).start()

    def finish1(kk, th, spot):
        for direction in range(2):
            copy1(kk, th, 1, direction, spot).wait_recv()
        for direction in range(2):
            copy1(kk, th, 2, direction, spot).wait_recv()
        sums = []
        for half in range(2):
            sums.append(
                own[kk, th, spot, half_rows(half), :]
                + recv1[kk, th, 2, half, spot].astype(F32)
                + recv1[kk, th, 1, 1 - half, spot].astype(F32)
            )
        return sums

    def stage2_start(th):
        for kk in range(2):
            low, high = finish1(kk, th, 0)
            send2[kk, th, 1, half_rows(0), :] = low.astype(BF16)
            send2[kk, th, 1, half_rows(1), :] = high.astype(BF16)
            copy2(kk, th, 0, 0).start()
            copy2(kk, th, 0, 1).start()
        for kk in range(2):
            low, high = finish1(kk, th, 1)
            own[kk, th, 1, half_rows(0), :] = low
            send2[kk, th, 0, half_rows(1), :] = high.astype(BF16)
            copy2(kk, th, 1, 0).start()
            low, high = finish1(kk, th, 2)
            send2[kk, th, 2, half_rows(0), :] = low.astype(BF16)
            own[kk, th, 2, half_rows(1), :] = high
            copy2(kk, th, 1, 1).start()

    def accumulate2(th):
        for kk, direction in pairs:
            copy2(kk, th, 0, direction).wait_recv()
            spot = 1 + direction
            total = own[kk, th, spot, half_rows(direction), :] + recv2[kk, th, 0, direction].astype(F32)
            send2[kk, th, 0 if direction == 0 else 2, half_rows(direction), :] = total.astype(BF16)
            copy2(kk, th, 2, direction).start()

    def exchange(th):
        for kk in range(2):
            sums = finish1(kk, th, 3)
            for kind in (1, 2):
                for direction in range(2):
                    copy2(kk, th, kind, direction).wait_recv()
            for half in range(2):
                total = sums[half] + recv2[kk, th, 2, half].astype(F32) + recv2[kk, th, 1, 1 - half].astype(F32)
                seen = obsbuf[kk, half_rows(half), th * LANES:(th + 1) * LANES].astype(F32)
                sums[half] = (total - seen).astype(BF16)
            residual = jnp.concatenate(sums, axis=0)
            packed = jnp.dot(sel[...], residual, preferred_element_type=F32).astype(BF16)
            send3[kk, th] = packed
            for off in (4, 3, 5, 2, 6, 1, 7):
                copy3(kk, th, off).start()
            here = pl.ds(pl.multiple_of(rcv * CAP, CAP), CAP)
            recv3[kk, th, here, :] = send3[kk, th, here, :]

    def inject(th):
        for kk in range(2):
            for off in range(1, BLOCKS):
                copy3(kk, th, off).wait_recv()
            obuf[kk, :, th * LANES:(th + 1) * LANES] = jnp.dot(
                injc[...], recv3[kk, th], preferred_element_type=F32
            )

    loads[1].wait()
    encode(0, 0)
    loads[2].wait()
    encode(0, 1)
    pl.semaphore_wait(barrier, 4 + BLOCKS - 1)
    start1(0, 0, (0, 1, 2, 3), (0,))
    start1(0, 1, (0, 1), (1,))
    loads[3].wait()
    encode(1, 2)
    loads[4].wait()
    encode(1, 3)
    start1(0, 0, (0, 1, 2, 3), (1,))
    start1(0, 1, (0, 1, 2), (0,))
    start1(0, 1, (2,), (1,))

    for load in loads[5:]:
        load.wait()
    before = (iota((RCV, RCV), 0) < iota((RCV, RCV), 1)).astype(BF16)

    def rank_of(window):
        named = (iota((BLOCKS, RCV), 0) == window).astype(F32)
        count = jnp.dot(named.astype(BF16), before, preferred_element_type=F32)
        return jnp.sum(named * count, axis=0, keepdims=True).astype(I32)

    mine = blk[:, pl.ds(pl.multiple_of(rcv * RCV, RCV), RCV)]
    sel[...] = (iota((BLOCKS * CAP, RCV), 0) == mine * CAP + rank_of(mine)).astype(BF16)
    for pair in range(BLOCKS // 2):
        chosen = []
        for side in range(2):
            start = (2 * pair + side) * RCV
            window = blk[:, start:start + RCV]
            slot = jnp.where(window == rcv, side * CAP + rank_of(window), -1)
            chosen.append((iota((2 * CAP, RCV), 0) == slot).astype(BF16))
            spread = jnp.zeros((GRID, RCV), F32)
            for which in range(STENCIL):
                point = idx[which:which + 1, start:start + RCV]
                weight = wgt[which:which + 1, start:start + RCV]
                spread = spread + jnp.where(iota((GRID, RCV), 0) == point, weight, 0.0)
            inj[:, side * RCV:(side + 1) * RCV] = spread.astype(BF16)
        injc[:, pair * LANES:(pair + 1) * LANES] = lax.dot_general(
            inj[...], jnp.concatenate(chosen, axis=1), (((1,), (1,)), ((), ())), preferred_element_type=F32
        ).astype(BF16)

    for spot in (0, 1, 2):
        accumulate1(0, spot)
    start1(1, 0, (0, 1, 2, 3))
    stage2_start(0)
    start1(1, 1, (0, 1, 2))
    accumulate2(0)
    for spot in (0, 1, 2):
        accumulate1(1, spot)
    start1(0, 1, (3,))
    accumulate1(0, 3)
    stage2_start(1)
    start1(1, 1, (3,))
    accumulate1(1, 3)
    exchange(0)
    accumulate2(1)
    exchange(1)
    inject(0)
    inject(1)
    put = pltpu.make_async_copy(obuf, out_hbm, out_sem)
    put.start()
    for kk, direction in pairs:
        for th in range(2):
            for kind in range(3):
                for spot in range(4):
                    copy1(kk, th, kind, direction, spot).wait_send()
                copy2(kk, th, kind, direction).wait_send()
    for kk in range(2):
        for th in range(2):
            for off in range(1, BLOCKS):
                copy3(kk, th, off).wait_send()
    put.wait()


def local(shot_data, code, observed, block_of, stencil_index, stencil_weight):
    dma = pltpu.SemaphoreType.DMA
    any_space = pl.BlockSpec(memory_space=pl.ANY)
    return pl.pallas_call(
        kernel,
        out_shape=jax.ShapeDtypeStruct((2, GRID, SAMPLES), F32),
        in_specs=[any_space] * 6,
        out_specs=any_space,
        scratch_shapes=[
            pltpu.VMEM((SHOTS_DEV, RCV, SAMPLES), BF16),
            pltpu.VMEM((SUPERS, SHOTS_DEV), I32),
            pltpu.VMEM((2, RCV, SAMPLES), BF16),
            pltpu.VMEM((1, BLOCKS * RCV), I32),
            pltpu.VMEM((STENCIL, BLOCKS * RCV), I32),
            pltpu.VMEM((STENCIL, BLOCKS * RCV), F32),
            pltpu.VMEM((ROWS, DEPTH), BF16),
            pltpu.VMEM((GRID, 2 * RCV), BF16),
            pltpu.VMEM((GRID, BLOCKS * CAP), BF16),
            pltpu.VMEM((BLOCKS * CAP, RCV), BF16),
            pltpu.VMEM((2, GRID, SAMPLES), F32),
            pltpu.VMEM((2, 2, 4, RCV, LANES), F32),
            pltpu.VMEM((2, 2, 2, 4, HALF, LANES), F32),
            pltpu.VMEM((2, 2, 3, 4, RCV, LANES), BF16),
            pltpu.VMEM((2, 2, 3, 2, 4, HALF, LANES), BF16),
            pltpu.VMEM((2, 2, 3, RCV, LANES), BF16),
            pltpu.VMEM((2, 2, 3, 2, HALF, LANES), BF16),
            pltpu.VMEM((2, 2, BLOCKS * CAP, LANES), BF16),
            pltpu.VMEM((2, 2, BLOCKS * CAP, LANES), BF16),
            dma((9,)),
            dma,
            dma((2, 2, 3, 2, 4)),
            dma((2, 2, 3, 2, 4)),
            dma((2, 2, 3, 2)),
            dma((2, 2, 3, 2)),
            dma((2, 2, BLOCKS - 1)),
            dma((2, 2, BLOCKS - 1)),
        ],
        compiler_params=pltpu.CompilerParams(
            collective_id=0, has_side_effects=True, vmem_limit_bytes=60 * 1024 * 1024
        ),
    )(shot_data, code, observed, block_of.T, stencil_index.T, stencil_weight.T)


def solution(mesh):
    split = P("shot", "rcv", None)
    return jax.shard_map(
        local,
        mesh=mesh,
        in_specs=(split, P(None, "shot"), split, P(), P(), P()),
        out_specs=split,
        check_vma=False,
    )
```

```python
import jax
import jax.numpy as jnp
from jax import lax
from jax.experimental import pallas as pl
from jax.experimental.pallas import tpu as pltpu
from jax.sharding import PartitionSpec as P

SUPERS = 32
GRID = 256
STENCIL = 4
BLOCKS = 8
CAP = 64
RING = 4
RCV = 256
HALF = RCV // 2
SAMPLES = 256
LANES = 128
SHOTS_DEV = 32
GROUP = 16
ROWS = SUPERS * GROUP
DEPTH = SHOTS_DEV * GROUP
ORDER = (2, 1, 3, 0)
F32, BF16, I32 = jnp.float32, jnp.bfloat16, jnp.int32
MESH = pl.DeviceIdType.MESH
SCHEDULE = (
    ("plain", 1, 0, 1), ("relay", 0, 1, 0), ("relay", 1, 1, 0), ("relay", 1, 1, 2),
    ("plain", 0, 0, 1), ("relay", 0, 1, 1), ("relay", 0, 1, 2), ("plain", 1, 0, 0),
    ("plain", 1, 0, 2), ("add", 0, 0, 0), ("add", 1, 0, 0), ("relay", 1, 1, 1),
    ("plain", 0, 0, 0), ("plain", 0, 1, 0), ("add", 0, 0, 1), ("add", 1, 0, 1),
    ("plain", 1, 1, 1), ("plain", 0, 0, 2), ("add", 0, 1, 0), ("plain", 1, 1, 0),
    ("add", 1, 0, 2), ("add", 1, 1, 0), ("plain", 0, 1, 1), ("add", 0, 0, 2),
    ("plain", 0, 1, 2), ("turn", 1, 0, 0), ("turn", 0, 0, 0), ("add", 1, 1, 1),
    ("add", 0, 1, 1), ("relay", 1, 1, 3), ("plain", 1, 1, 2), ("add", 0, 1, 2),
    ("turn", 0, 1, 0), ("add", 1, 1, 2), ("relay", 0, 1, 3), ("add", 0, 0, 3),
    ("turn", 0, 0, 2), ("turn", 1, 1, 0), ("plain", 0, 0, 3), ("turn", 1, 0, 2),
    ("turn", 0, 0, 1), ("add2", 0, 0), ("turn", 1, 0, 1), ("add2", 1, 0),
    ("add", 1, 0, 3), ("plain", 1, 0, 3), ("turn", 0, 1, 1), ("plain", 0, 1, 3),
    ("turn", 0, 1, 2), ("add", 0, 1, 3), ("turn", 1, 1, 1), ("add2", 0, 1),
    ("turn", 1, 1, 2), ("plain", 1, 1, 3), ("add2", 1, 1), ("add", 1, 1, 3),
    ("swap", 0, 0), ("swap", 1, 0), ("swap", 0, 1), ("swap", 1, 1),
)


def iota(shape, dim):
    return lax.broadcasted_iota(I32, shape, dim)


def encoding_rows(shape, y, z):
    row = iota(shape, 0)
    kk = row // (ROWS // 2)
    first = (row // (4 * GROUP)) % 4
    spot = (row // GROUP) % 4
    second = jnp.where(spot == 0, 2, jnp.where(spot == 1, 1, jnp.where(spot == 2, 3, 0)))
    dy = jnp.where(kk == 0, first, second)
    dz = jnp.where(kk == 0, second, first)
    return 8 * ((y + dy) % 4) + 2 * ((z + dz) % 4) + kk


def kernel(
    shot_hbm, code_hbm, obs_hbm, blk_hbm, idx_hbm, wgt_hbm, out,
    xbuf, codebuf, obsbuf, blk, idx, wgt, enc, inj, injc, sel,
    own, keep, send1, send2, send3, got_relay, got_turn, got_last, got_relay2, got_swap,
    load_sem, s_relay, s_turn, s_last, s_relay2, s_swap, r_relay, r_turn, r_last, r_relay2, r_swap,
):
    shot, rcv = lax.axis_index("shot"), lax.axis_index("rcv")
    y, z = shot // 4, shot % 4

    def at_shot(dy, dz):
        return (((y + dy) % 4) * 4 + (z + dz) % 4, rcv)

    def neighbour(kk, stage, direction):
        step = 1 if direction == 0 else 3
        along_y = (kk == 0) == (stage == 1)
        return at_shot(step, 0) if along_y else at_shot(0, step)

    loads = [pltpu.make_async_copy(code_hbm, codebuf, load_sem.at[0])]
    for chunk in range(4):
        rows = pl.ds(chunk * 64, 64)
        loads.append(pltpu.make_async_copy(shot_hbm.at[:, rows], xbuf.at[:, rows], load_sem.at[1 + chunk]))
    loads.append(pltpu.make_async_copy(obs_hbm, obsbuf, load_sem.at[5]))
    loads.append(pltpu.make_async_copy(blk_hbm, blk, load_sem.at[6]))
    loads.append(pltpu.make_async_copy(idx_hbm, idx, load_sem.at[7]))
    loads.append(pltpu.make_async_copy(wgt_hbm, wgt, load_sem.at[8]))
    for load in loads:
        load.start()

    barrier = pltpu.get_barrier_semaphore()
    for peer in (at_shot(1, 0), at_shot(3, 0), at_shot(0, 1), at_shot(0, 3)):
        pl.semaphore_signal(barrier, inc=1, device_id=peer, device_id_type=MESH)
    for off in range(1, BLOCKS):
        pl.semaphore_signal(barrier, inc=1, device_id=(shot, (rcv + off) % BLOCKS), device_id_type=MESH)

    loads[0].wait()
    pick = (encoding_rows((ROWS, SUPERS), y, z) == iota((ROWS, SUPERS), 1)).astype(BF16)
    codes = jnp.dot(pick, codebuf[...].astype(F32).astype(BF16), preferred_element_type=F32).astype(BF16)
    widen = (iota((SHOTS_DEV, DEPTH), 1) // GROUP == iota((SHOTS_DEV, DEPTH), 0)).astype(BF16)
    wide = jnp.dot(codes, widen, preferred_element_type=F32)
    same = iota((ROWS, DEPTH), 0) % GROUP == iota((ROWS, DEPTH), 1) % GROUP
    enc[...] = jnp.where(same, wide, 0.0).astype(BF16)

    def half_rows(half):
        return pl.ds(half * HALF, HALF)

    def encode(half, chunk):
        def body(step, carry):
            r0 = pl.multiple_of(chunk * 64 + step * GROUP, GROUP)
            data = xbuf[:, pl.ds(r0, GROUP), :].reshape(DEPTH, SAMPLES)
            for kk in range(2):
                product = jnp.dot(enc[kk * 256:(kk + 1) * 256, :], data, preferred_element_type=F32)
                product = product.reshape(4, 4, GROUP, SAMPLES)
                for th in range(2):
                    part = product[:, :, :, th * LANES:(th + 1) * LANES]
                    rows = pl.ds(r0, GROUP)
                    inner = pl.ds(pl.multiple_of(r0 - half * HALF, GROUP), GROUP)
                    own[kk, th, :, rows, :] = part[0]
                    send1[kk, th, 1, :, rows, :] = part[2].astype(BF16)
                    if half == 0:
                        keep[kk, th, 0, :, inner, :] = part[1]
                        send1[kk, th, 2, :, rows, :] = part[3].astype(BF16)
                    else:
                        send1[kk, th, 0, :, rows, :] = part[1].astype(BF16)
                        keep[kk, th, 1, :, inner, :] = part[3]
            return carry

        lax.fori_loop(0, 4, body, 0, unroll=True)

    def copy1(kk, th, kind, direction, spot):
        unit = 2 * kk + th
        slot = 1 if kind == 0 else (0 if direction == 0 else 2)
        half = direction if kind in (0, 2) else 1 - direction
        if kind == 0:
            place, sems = got_relay.at[unit * 4 + spot, direction], (s_relay, r_relay.at[unit * 4 + spot])
        elif spot < 3:
            place, sems = got_turn.at[unit * 3 + spot, 2 * (kind - 1) + direction], (s_turn, r_turn.at[unit * 3 + spot])
        else:
            place, sems = got_last.at[unit, 2 * (kind - 1) + direction], (s_last, r_last.at[unit])
        return pltpu.make_async_remote_copy(
            src_ref=send1.at[kk, th, slot, spot, half_rows(half)],
            dst_ref=place,
            send_sem=sems[0],
            recv_sem=sems[1],
            device_id=neighbour(kk, 1, direction),
            device_id_type=MESH,
        )

    def copy2(kk, th, kind, direction):
        unit = 2 * kk + th
        slot = 1 if kind == 0 else (0 if direction == 0 else 2)
        half = direction if kind in (0, 2) else 1 - direction
        if kind == 0:
            place, sems = got_relay2.at[unit, direction], (s_relay2, r_relay2.at[unit])
        else:
            place, sems = got_last.at[unit, 2 + 2 * kind + direction], (s_last, r_last.at[unit])
        return pltpu.make_async_remote_copy(
            src_ref=send2.at[kk, th, slot, half_rows(half)],
            dst_ref=place,
            send_sem=sems[0],
            recv_sem=sems[1],
            device_id=neighbour(kk, 2, direction),
            device_id_type=MESH,
        )

    def copy3(kk, th, off):
        block = (rcv + off) % BLOCKS
        return pltpu.make_async_remote_copy(
            src_ref=send3.at[kk, th, pl.ds(pl.multiple_of(block * CAP, CAP), CAP)],
            dst_ref=got_swap.at[2 * kk + th, pl.ds(pl.multiple_of(rcv * CAP, CAP), CAP)],
            send_sem=s_swap,
            recv_sem=r_swap.at[2 * kk + th],
            device_id=(shot, block),
            device_id_type=MESH,
        )

    def arrived(place, sem):
        pltpu.make_async_copy(place, place, sem).wait()

    def relay(kk, th, spot, directions=(0, 1)):
        for direction in directions:
            copy1(kk, th, 0, direction, spot).start()

    def plain(kk, th, spot, directions=(0, 1)):
        for direction in directions:
            copy1(kk, th, 1, direction, spot).start()

    def add(kk, th, spot):
        at = (2 * kk + th) * 4 + spot
        arrived(got_relay.at[at], r_relay.at[at])
        for direction in range(2):
            total = keep[kk, th, direction, spot] + got_relay[at, direction].astype(F32)
            send1[kk, th, 0 if direction == 0 else 2, spot, half_rows(direction), :] = total.astype(BF16)
            copy1(kk, th, 2, direction, spot).start()

    def summed(kk, th, spot, plain_at, added_at):
        return [
            own[kk, th, spot, half_rows(half), :] + added_at[half].astype(F32) + plain_at[1 - half].astype(F32)
            for half in range(2)
        ]

    def turn(kk, th, spot):
        at = (2 * kk + th) * 3 + spot
        arrived(got_turn.at[at], r_turn.at[at])
        low, high = summed(
            kk, th, spot, [got_turn[at, 0], got_turn[at, 1]], [got_turn[at, 2], got_turn[at, 3]]
        )
        if spot == 0:
            send2[kk, th, 1, half_rows(0), :] = low.astype(BF16)
            send2[kk, th, 1, half_rows(1), :] = high.astype(BF16)
            copy2(kk, th, 0, 0).start()
            copy2(kk, th, 0, 1).start()
        elif spot == 1:
            own[kk, th, 1, half_rows(0), :] = low
            send2[kk, th, 0, half_rows(1), :] = high.astype(BF16)
            copy2(kk, th, 1, 0).start()
        else:
            send2[kk, th, 2, half_rows(0), :] = low.astype(BF16)
            own[kk, th, 2, half_rows(1), :] = high
            copy2(kk, th, 1, 1).start()

    def add2(kk, th):
        unit = 2 * kk + th
        arrived(got_relay2.at[unit], r_relay2.at[unit])
        for direction in range(2):
            total = own[kk, th, 1 + direction, half_rows(direction), :] + got_relay2[unit, direction].astype(F32)
            send2[kk, th, 0 if direction == 0 else 2, half_rows(direction), :] = total.astype(BF16)
            copy2(kk, th, 2, direction).start()

    def swap(kk, th):
        unit = 2 * kk + th
        arrived(got_last.at[unit], r_last.at[unit])
        last = [got_last[unit, part] for part in range(8)]
        sums = summed(kk, th, 3, last[0:2], last[2:4])
        for half in range(2):
            total = sums[half] + last[6 + half].astype(F32) + last[5 - half].astype(F32)
            seen = obsbuf[kk, half_rows(half), th * LANES:(th + 1) * LANES].astype(F32)
            sums[half] = (total - seen).astype(BF16)
        residual = jnp.concatenate(sums, axis=0)
        packed = jnp.dot(sel[...], residual, preferred_element_type=F32).astype(BF16)
        send3[kk, th] = packed
        for off in (4, 3, 5, 2, 6, 1, 7):
            copy3(kk, th, off).start()
        here = pl.ds(pl.multiple_of(rcv * CAP, CAP), CAP)
        got_swap[unit, here, :] = send3[kk, th, here, :]

    def inject(kk, th):
        unit = 2 * kk + th
        arrived(got_swap.at[unit, pl.ds(0, (BLOCKS - 1) * CAP)], r_swap.at[unit])
        out[kk, :, th * LANES:(th + 1) * LANES] = jnp.dot(
            injc[...], got_swap[unit], preferred_element_type=F32
        )

    def tables():
        for load in loads[5:]:
            load.wait()
        before = (iota((RCV, RCV), 0) < iota((RCV, RCV), 1)).astype(BF16)

        def rank_of(window):
            named = (iota((BLOCKS, RCV), 0) == window).astype(F32)
            count = jnp.dot(named.astype(BF16), before, preferred_element_type=F32)
            return jnp.sum(named * count, axis=0, keepdims=True).astype(I32)

        mine = blk[:, pl.ds(pl.multiple_of(rcv * RCV, RCV), RCV)]
        sel[...] = (iota((BLOCKS * CAP, RCV), 0) == mine * CAP + rank_of(mine)).astype(BF16)
        for pair in range(BLOCKS // 2):
            chosen = []
            for side in range(2):
                start = (2 * pair + side) * RCV
                window = blk[:, start:start + RCV]
                slot = jnp.where(window == rcv, side * CAP + rank_of(window), -1)
                chosen.append((iota((2 * CAP, RCV), 0) == slot).astype(BF16))
                spread = jnp.zeros((GRID, RCV), F32)
                for which in range(STENCIL):
                    point = idx[which:which + 1, start:start + RCV]
                    weight = wgt[which:which + 1, start:start + RCV]
                    spread = spread + jnp.where(iota((GRID, RCV), 0) == point, weight, 0.0)
                inj[:, side * RCV:(side + 1) * RCV] = spread.astype(BF16)
            injc[:, pair * LANES:(pair + 1) * LANES] = lax.dot_general(
                inj[...], jnp.concatenate(chosen, axis=1), (((1,), (1,)), ((), ())), preferred_element_type=F32
            ).astype(BF16)

    loads[1].wait()
    encode(0, 0)
    loads[2].wait()
    encode(0, 1)
    pl.semaphore_wait(barrier, 4 + BLOCKS - 1)
    for spot in range(4):
        for kk in range(2):
            relay(kk, 0, spot, (0,))
    for spot in range(2):
        for kk in range(2):
            plain(kk, 0, spot, (1,))
    loads[3].wait()
    encode(1, 2)
    loads[4].wait()
    encode(1, 3)
    for spot in range(4):
        for kk in range(2):
            relay(kk, 0, spot, (1,))

    steps = {"relay": relay, "plain": plain, "add": add, "turn": turn, "add2": add2, "swap": swap}
    waiting = False
    for name, kk, th, *spot in SCHEDULE:
        if name not in ("relay", "plain") and not waiting:
            tables()
            waiting = True
        if name == "plain" and th == 0 and spot[0] < 2:
            plain(kk, 0, spot[0], (0,))
        else:
            steps[name](kk, th, *spot)
    for name, kk, th in SCHEDULE[-4:]:
        inject(kk, th)
    arrived(got_relay, s_relay)
    arrived(got_turn, s_turn)
    arrived(got_last, s_last)
    arrived(got_relay2, s_relay2)
    arrived(got_relay.at[pl.ds(0, BLOCKS - 1)], s_swap)


def local(shot_data, code, observed, block_of, stencil_index, stencil_weight):
    dma = pltpu.SemaphoreType.DMA
    any_space = pl.BlockSpec(memory_space=pltpu.HBM)
    return pl.pallas_call(
        kernel,
        out_shape=jax.ShapeDtypeStruct((2, GRID, SAMPLES), F32),
        in_specs=[any_space] * 6,
        out_specs=pl.BlockSpec(memory_space=pltpu.VMEM),
        scratch_shapes=[
            pltpu.VMEM((SHOTS_DEV, RCV, SAMPLES), BF16),
            pltpu.VMEM((SUPERS, SHOTS_DEV), I32),
            pltpu.VMEM((2, RCV, SAMPLES), BF16),
            pltpu.VMEM((1, BLOCKS * RCV), I32),
            pltpu.VMEM((STENCIL, BLOCKS * RCV), I32),
            pltpu.VMEM((STENCIL, BLOCKS * RCV), F32),
            pltpu.VMEM((ROWS, DEPTH), BF16),
            pltpu.VMEM((GRID, 2 * RCV), BF16),
            pltpu.VMEM((GRID, BLOCKS * CAP), BF16),
            pltpu.VMEM((BLOCKS * CAP, RCV), BF16),
            pltpu.VMEM((2, 2, 4, RCV, LANES), F32),
            pltpu.VMEM((2, 2, 2, 4, HALF, LANES), F32),
            pltpu.VMEM((2, 2, 3, 4, RCV, LANES), BF16),
            pltpu.VMEM((2, 2, 3, RCV, LANES), BF16),
            pltpu.VMEM((2, 2, BLOCKS * CAP, LANES), BF16),
            pltpu.VMEM((16, 2, HALF, LANES), BF16),
            pltpu.VMEM((12, 4, HALF, LANES), BF16),
            pltpu.VMEM((4, 8, HALF, LANES), BF16),
            pltpu.VMEM((4, 2, HALF, LANES), BF16),
            pltpu.VMEM((4, BLOCKS * CAP, LANES), BF16),
            dma((9,)),
            dma,
            dma,
            dma,
            dma,
            dma,
            dma((16,)),
            dma((12,)),
            dma((4,)),
            dma((4,)),
            dma((4,)),
        ],
        compiler_params=pltpu.CompilerParams(
            collective_id=0, has_side_effects=True, vmem_limit_bytes=52 * 1024 * 1024
        ),
    )(*[pltpu.with_memory_space_constraint(v, pltpu.HBM) for v in (shot_data, code, observed, block_of.T, stencil_index.T, stencil_weight.T)])


def solution(mesh):
    split = P("shot", "rcv", None)
    return jax.shard_map(
        local,
        mesh=mesh,
        in_specs=(split, P(None, "shot"), split, P(), P(), P()),
        out_specs=split,
        check_vma=False,
    )
```

```python
import jax
import jax.numpy as jnp
from jax import lax
from jax.experimental import pallas as pl
from jax.experimental.pallas import tpu as pltpu
from jax.sharding import PartitionSpec as P

SUPERS = 32
GRID = 256
STENCIL = 4
BLOCKS = 8
CAP = 64
RING = 4
RCV = 256
HALF = RCV // 2
SAMPLES = 256
LANES = 128
SHOTS_DEV = 32
GROUP = 16
ROWS = SUPERS * GROUP
DEPTH = SHOTS_DEV * GROUP
ORDER = (2, 1, 3, 0)
F32, BF16, I32 = jnp.float32, jnp.bfloat16, jnp.int32
MESH = pl.DeviceIdType.MESH
SCHEDULE = (
    ("relay", 1, 1, 0), ("plain", 0, 0, 0), ("relay", 0, 1, 0), ("plain", 0, 0, 1),
    ("plain", 1, 0, 0), ("plain", 1, 0, 1), ("plain", 1, 0, 2), ("relay", 0, 1, 2),
    ("plain", 1, 1, 0), ("relay", 1, 1, 3), ("plain", 0, 1, 0), ("plain", 0, 0, 2),
    ("add", 0, 0, 0), ("relay", 0, 1, 1), ("relay", 1, 1, 1), ("add", 1, 0, 0),
    ("relay", 1, 1, 2), ("add", 0, 0, 1), ("plain", 1, 1, 1), ("add", 1, 0, 2),
    ("add", 0, 0, 2), ("add", 1, 1, 0), ("add", 0, 1, 0), ("add", 0, 1, 2),
    ("relay", 0, 1, 3), ("add", 1, 0, 1), ("turn", 0, 0, 0), ("plain", 0, 1, 1),
    ("plain", 1, 1, 2), ("add", 0, 1, 1), ("turn", 1, 0, 0), ("add", 1, 1, 2),
    ("add", 1, 1, 1), ("plain", 0, 1, 2), ("turn", 0, 1, 0), ("turn", 0, 0, 2),
    ("plain", 0, 0, 3), ("turn", 1, 1, 0), ("add", 0, 0, 3), ("turn", 0, 0, 1),
    ("turn", 1, 0, 1), ("add2", 0, 0), ("plain", 1, 0, 3), ("turn", 1, 0, 2),
    ("add", 1, 0, 3), ("add2", 1, 0), ("add", 0, 1, 3), ("plain", 0, 1, 3),
    ("turn", 0, 1, 1), ("turn", 1, 1, 2), ("turn", 0, 1, 2), ("add2", 0, 1),
    ("plain", 1, 1, 3), ("turn", 1, 1, 1), ("add2", 1, 1), ("add", 1, 1, 3),
    ("swap", 0, 0), ("swap", 1, 0), ("swap", 0, 1), ("swap", 1, 1),
)


def iota(shape, dim):
    return lax.broadcasted_iota(I32, shape, dim)


def encoding_rows(shape, y, z):
    row = iota(shape, 0)
    kk = row // 16
    first = (row // 4) % 4
    spot = row % 4
    second = jnp.where(spot == 0, 2, jnp.where(spot == 1, 1, jnp.where(spot == 2, 3, 0)))
    dy = jnp.where(kk == 0, first, second)
    dz = jnp.where(kk == 0, second, first)
    return 8 * ((y + dy) % 4) + 2 * ((z + dz) % 4) + kk


def kernel(
    shot_hbm, code_hbm, obs_hbm, blk_hbm, idx_hbm, wgt_hbm, out,
    xbuf, codebuf, obsbuf, blk, idx, wgt, enc, inj, injc, sel,
    own, keep, send1, send2, send3, got_relay, got_turn, got_last, got_relay2, got_swap,
    load_sem, s_relay, s_turn, s_last, s_relay2, s_swap, r_relay, r_turn, r_last, r_relay2, r_swap,
):
    shot, rcv = lax.axis_index("shot"), lax.axis_index("rcv")
    y, z = shot // 4, shot % 4

    def at_shot(dy, dz):
        return (((y + dy) % 4) * 4 + (z + dz) % 4, rcv)

    def neighbour(kk, stage, direction):
        step = 1 if direction == 0 else 3
        along_y = (kk == 0) == (stage == 1)
        return at_shot(step, 0) if along_y else at_shot(0, step)

    barrier = pltpu.get_barrier_semaphore()
    for peer in (at_shot(1, 0), at_shot(3, 0), at_shot(0, 1), at_shot(0, 3)):
        pl.semaphore_signal(barrier, inc=1, device_id=peer, device_id_type=MESH)
    for off in range(1, BLOCKS):
        pl.semaphore_signal(barrier, inc=1, device_id=(shot, (rcv + off) % BLOCKS), device_id_type=MESH)

    loads = [pltpu.make_async_copy(code_hbm, codebuf, load_sem.at[0])]
    for chunk in range(4):
        rows = pl.ds(chunk * 64, 64)
        loads.append(pltpu.make_async_copy(shot_hbm.at[:, rows], xbuf.at[:, rows], load_sem.at[1 + chunk]))
    loads.append(pltpu.make_async_copy(obs_hbm, obsbuf, load_sem.at[5]))
    loads.append(pltpu.make_async_copy(blk_hbm, blk, load_sem.at[6]))
    loads.append(pltpu.make_async_copy(idx_hbm, idx, load_sem.at[7]))
    loads.append(pltpu.make_async_copy(wgt_hbm, wgt, load_sem.at[8]))
    for load in loads:
        load.start()

    pick = (encoding_rows((SUPERS, SUPERS), y, z) == iota((SUPERS, SUPERS), 1)).astype(BF16)
    widen = (iota((SHOTS_DEV, DEPTH), 1) // GROUP == iota((SHOTS_DEV, DEPTH), 0)).astype(BF16)
    same = iota((1, GROUP, DEPTH), 1) == iota((1, GROUP, DEPTH), 2) % GROUP
    loads[0].wait()
    codes = jnp.dot(pick, codebuf[...].astype(F32).astype(BF16), preferred_element_type=F32).astype(BF16)
    wide = jnp.dot(codes, widen, preferred_element_type=F32)
    enc[...] = jnp.where(same, wide[:, None, :], 0.0).astype(BF16).reshape(ROWS, DEPTH)

    def half_rows(half):
        return pl.ds(half * HALF, HALF)

    def encode(chunk):
        half = chunk // 2
        for step in range(4):
            r0 = chunk * 64 + step * GROUP
            data = xbuf[:, r0:r0 + GROUP, :].reshape(DEPTH, SAMPLES)
            rows, inner = pl.ds(r0, GROUP), pl.ds(r0 - half * HALF, GROUP)
            for kk in range(2):
                product = jnp.dot(enc[kk * 256:(kk + 1) * 256, :], data, preferred_element_type=F32)
                product = product.reshape(4, 4, GROUP, SAMPLES)
                for th in range(2):
                    part = product[:, :, :, th * LANES:(th + 1) * LANES]
                    own[kk, th, :, rows, :] = part[0]
                    send1[kk, th, 1, :, rows, :] = part[2].astype(BF16)
                    if half == 0:
                        keep[kk, th, 0, :, inner, :] = part[1]
                        send1[kk, th, 2, :, rows, :] = part[3].astype(BF16)
                    else:
                        send1[kk, th, 0, :, rows, :] = part[1].astype(BF16)
                        keep[kk, th, 1, :, inner, :] = part[3]

    def copy1(kk, th, kind, direction, spot, part_at=None):
        unit = 2 * kk + th
        slot = 1 if kind == 0 else (0 if direction == 0 else 2)
        half = direction if kind in (0, 2) else 1 - direction
        if kind == 0:
            place, sems = got_relay.at[unit * 4 + spot, direction], (s_relay, r_relay.at[unit * 4 + spot])
        elif spot < 3:
            place, sems = got_turn.at[unit * 3 + spot, 2 * (kind - 1) + direction], (s_turn, r_turn.at[unit * 3 + spot])
        else:
            place, sems = got_last.at[unit, 2 * (kind - 1) + direction], (s_last, r_last.at[unit])
        rows = half_rows(half)
        if part_at is not None:
            rows, place = pl.ds(half * HALF + part_at * 64, 64), place.at[pl.ds(part_at * 64, 64)]
        return pltpu.make_async_remote_copy(
            src_ref=send1.at[kk, th, slot, spot, rows],
            dst_ref=place,
            send_sem=sems[0],
            recv_sem=sems[1],
            device_id=neighbour(kk, 1, direction),
            device_id_type=MESH,
        )

    def copy2(kk, th, kind, direction):
        unit = 2 * kk + th
        slot = 1 if kind == 0 else (0 if direction == 0 else 2)
        half = direction if kind in (0, 2) else 1 - direction
        if kind == 0:
            place, sems = got_relay2.at[unit, direction], (s_relay2, r_relay2.at[unit])
        else:
            place, sems = got_last.at[unit, 2 + 2 * kind + direction], (s_last, r_last.at[unit])
        return pltpu.make_async_remote_copy(
            src_ref=send2.at[kk, th, slot, half_rows(half)],
            dst_ref=place,
            send_sem=sems[0],
            recv_sem=sems[1],
            device_id=neighbour(kk, 2, direction),
            device_id_type=MESH,
        )

    def copy3(kk, th, off):
        block = (rcv + off) % BLOCKS
        return pltpu.make_async_remote_copy(
            src_ref=send3.at[kk, th, pl.ds(pl.multiple_of(block * CAP, CAP), CAP)],
            dst_ref=got_swap.at[2 * kk + th, pl.ds(pl.multiple_of(rcv * CAP, CAP), CAP)],
            send_sem=s_swap,
            recv_sem=r_swap.at[2 * kk + th],
            device_id=(shot, block),
            device_id_type=MESH,
        )

    def arrived(place, sem):
        pltpu.make_async_copy(place, place, sem).wait()

    def relay(kk, th, spot, directions=(0, 1), part_at=None):
        for direction in directions:
            copy1(kk, th, 0, direction, spot, part_at).start()

    def plain(kk, th, spot, directions=(0, 1), part_at=None):
        for direction in directions:
            copy1(kk, th, 1, direction, spot, part_at).start()

    def add(kk, th, spot):
        at = (2 * kk + th) * 4 + spot
        arrived(got_relay.at[at], r_relay.at[at])
        for direction in range(2):
            total = keep[kk, th, direction, spot] + got_relay[at, direction].astype(F32)
            send1[kk, th, 0 if direction == 0 else 2, spot, half_rows(direction), :] = total.astype(BF16)
            copy1(kk, th, 2, direction, spot).start()

    def summed(kk, th, spot, plain_at, added_at):
        return [
            own[kk, th, spot, half_rows(half), :] + added_at[half].astype(F32) + plain_at[1 - half].astype(F32)
            for half in range(2)
        ]

    def turn(kk, th, spot):
        at = (2 * kk + th) * 3 + spot
        arrived(got_turn.at[at], r_turn.at[at])
        low, high = summed(
            kk, th, spot, [got_turn[at, 0], got_turn[at, 1]], [got_turn[at, 2], got_turn[at, 3]]
        )
        if spot == 0:
            send2[kk, th, 1, half_rows(0), :] = low.astype(BF16)
            send2[kk, th, 1, half_rows(1), :] = high.astype(BF16)
            copy2(kk, th, 0, 0).start()
            copy2(kk, th, 0, 1).start()
        elif spot == 1:
            own[kk, th, 1, half_rows(0), :] = low
            send2[kk, th, 0, half_rows(1), :] = high.astype(BF16)
            copy2(kk, th, 1, 0).start()
        else:
            send2[kk, th, 2, half_rows(0), :] = low.astype(BF16)
            own[kk, th, 2, half_rows(1), :] = high
            copy2(kk, th, 1, 1).start()

    def add2(kk, th):
        unit = 2 * kk + th
        arrived(got_relay2.at[unit], r_relay2.at[unit])
        for direction in range(2):
            total = own[kk, th, 1 + direction, half_rows(direction), :] + got_relay2[unit, direction].astype(F32)
            send2[kk, th, 0 if direction == 0 else 2, half_rows(direction), :] = total.astype(BF16)
            copy2(kk, th, 2, direction).start()

    def swap(kk, th):
        unit = 2 * kk + th
        arrived(got_last.at[unit], r_last.at[unit])
        last = [got_last[unit, part] for part in range(8)]
        sums = summed(kk, th, 3, last[0:2], last[2:4])
        for half in range(2):
            total = sums[half] + last[6 + half].astype(F32) + last[5 - half].astype(F32)
            seen = obsbuf[kk, half_rows(half), th * LANES:(th + 1) * LANES].astype(F32)
            sums[half] = (total - seen).astype(BF16)
        residual = jnp.concatenate(sums, axis=0)
        packed = jnp.dot(sel[...], residual, preferred_element_type=F32).astype(BF16)
        send3[kk, th] = packed
        for off in (4, 3, 5, 2, 6, 1, 7):
            copy3(kk, th, off).start()
        here = pl.ds(pl.multiple_of(rcv * CAP, CAP), CAP)
        got_swap[unit, here, :] = send3[kk, th, here, :]

    def inject(kk, th):
        unit = 2 * kk + th
        arrived(got_swap.at[unit, pl.ds(0, (BLOCKS - 1) * CAP)], r_swap.at[unit])
        out[kk, :, th * LANES:(th + 1) * LANES] = jnp.dot(
            injc[...], got_swap[unit], preferred_element_type=F32
        )

    def tables():
        for load in loads[5:]:
            load.wait()
        before = (iota((RCV, RCV), 0) < iota((RCV, RCV), 1)).astype(BF16)

        def rank_of(window):
            named = (iota((BLOCKS, RCV), 0) == window).astype(F32)
            count = jnp.dot(named.astype(BF16), before, preferred_element_type=F32)
            return jnp.sum(named * count, axis=0, keepdims=True).astype(I32)

        mine = blk[:, pl.ds(pl.multiple_of(rcv * RCV, RCV), RCV)]
        sel[...] = (iota((BLOCKS * CAP, RCV), 0) == mine * CAP + rank_of(mine)).astype(BF16)
        for pair in range(BLOCKS // 2):
            chosen = []
            for side in range(2):
                start = (2 * pair + side) * RCV
                window = blk[:, start:start + RCV]
                slot = jnp.where(window == rcv, side * CAP + rank_of(window), -1)
                chosen.append((iota((2 * CAP, RCV), 0) == slot).astype(BF16))
                spread = jnp.zeros((GRID, RCV), F32)
                for which in range(STENCIL):
                    point = idx[which:which + 1, start:start + RCV]
                    weight = wgt[which:which + 1, start:start + RCV]
                    spread = spread + jnp.where(iota((GRID, RCV), 0) == point, weight, 0.0)
                inj[:, side * RCV:(side + 1) * RCV] = spread.astype(BF16)
            injc[:, pair * LANES:(pair + 1) * LANES] = lax.dot_general(
                inj[...], jnp.concatenate(chosen, axis=1), (((1,), (1,)), ((), ())), preferred_element_type=F32
            ).astype(BF16)

    for chunk in range(4):
        loads[1 + chunk].wait()
        encode(chunk)
        if chunk == 0:
            pl.semaphore_wait(barrier, 4 + BLOCKS - 1)
        for spot in range(4 if chunk < 2 else 2):
            for kk in range(2):
                relay(kk, 0, spot, (chunk // 2,), chunk % 2)
                if chunk < 2 and spot < 3:
                    plain(kk, 0, spot, (1,), chunk)
    for spot in range(2, 4):
        for kk in range(2):
            relay(kk, 0, spot, (1,))

    steps = {"relay": relay, "plain": plain, "add": add, "turn": turn, "add2": add2, "swap": swap}
    waiting = False
    for name, kk, th, *spot in SCHEDULE:
        if name not in ("relay", "plain") and not waiting:
            tables()
            waiting = True
        if name == "plain" and th == 0 and spot[0] < 3:
            plain(kk, 0, spot[0], (0,))
        else:
            steps[name](kk, th, *spot)
    for name, kk, th in [step for step in SCHEDULE if step[0] == "swap"]:
        inject(kk, th)
    arrived(got_relay, s_relay)
    arrived(got_turn, s_turn)
    arrived(got_last, s_last)
    arrived(got_relay2, s_relay2)
    arrived(got_relay.at[pl.ds(0, BLOCKS - 1)], s_swap)


def local(shot_data, code, observed, block_of, stencil_index, stencil_weight):
    dma = pltpu.SemaphoreType.DMA
    any_space = pl.BlockSpec(memory_space=pltpu.HBM)
    return pl.pallas_call(
        kernel,
        out_shape=jax.ShapeDtypeStruct((2, GRID, SAMPLES), F32),
        in_specs=[any_space] * 6,
        out_specs=pl.BlockSpec(memory_space=pltpu.VMEM),
        scratch_shapes=[
            pltpu.VMEM((SHOTS_DEV, RCV, SAMPLES), BF16),
            pltpu.VMEM((SUPERS, SHOTS_DEV), I32),
            pltpu.VMEM((2, RCV, SAMPLES), BF16),
            pltpu.VMEM((1, BLOCKS * RCV), I32),
            pltpu.VMEM((STENCIL, BLOCKS * RCV), I32),
            pltpu.VMEM((STENCIL, BLOCKS * RCV), F32),
            pltpu.VMEM((ROWS, DEPTH), BF16),
            pltpu.VMEM((GRID, 2 * RCV), BF16),
            pltpu.VMEM((GRID, BLOCKS * CAP), BF16),
            pltpu.VMEM((BLOCKS * CAP, RCV), BF16),
            pltpu.VMEM((2, 2, 4, RCV, LANES), F32),
            pltpu.VMEM((2, 2, 2, 4, HALF, LANES), F32),
            pltpu.VMEM((2, 2, 3, 4, RCV, LANES), BF16),
            pltpu.VMEM((2, 2, 3, RCV, LANES), BF16),
            pltpu.VMEM((2, 2, BLOCKS * CAP, LANES), BF16),
            pltpu.VMEM((16, 2, HALF, LANES), BF16),
            pltpu.VMEM((12, 4, HALF, LANES), BF16),
            pltpu.VMEM((4, 8, HALF, LANES), BF16),
            pltpu.VMEM((4, 2, HALF, LANES), BF16),
            pltpu.VMEM((4, BLOCKS * CAP, LANES), BF16),
            dma((9,)),
            dma,
            dma,
            dma,
            dma,
            dma,
            dma((16,)),
            dma((12,)),
            dma((4,)),
            dma((4,)),
            dma((4,)),
        ],
        compiler_params=pltpu.CompilerParams(
            collective_id=0, has_side_effects=True, vmem_limit_bytes=52 * 1024 * 1024
        ),
    )(*[pltpu.with_memory_space_constraint(v, pltpu.HBM) for v in (shot_data, code, observed, block_of.T, stencil_index.T, stencil_weight.T)])


def solution(mesh):
    split = P("shot", "rcv", None)
    return jax.shard_map(
        local,
        mesh=mesh,
        in_specs=(split, P(None, "shot"), split, P(), P(), P()),
        out_specs=split,
        check_vma=False,
    )
```

```python
import jax
import jax.numpy as jnp
from jax import lax
from jax.experimental import pallas as pl
from jax.experimental.pallas import tpu as pltpu
from jax.sharding import PartitionSpec as P

SUPERS = 32
GRID = 256
STENCIL = 4
BLOCKS = 8
CAP = 64
RING = 4
RCV = 256
HALF = RCV // 2
SAMPLES = 256
LANES = 128
SHOTS_DEV = 32
GROUP = 16
ROWS = SUPERS * GROUP
DEPTH = SHOTS_DEV * GROUP
ORDER = (2, 1, 3, 0)
F32, BF16, I32 = jnp.float32, jnp.bfloat16, jnp.int32
MESH = pl.DeviceIdType.MESH
SCHEDULE = (
    ("relay", 1, 1, 0), ("plain", 0, 0, 0), ("relay", 0, 1, 0), ("plain", 0, 0, 1),
    ("plain", 1, 0, 0), ("plain", 1, 0, 1), ("plain", 1, 0, 2), ("relay", 0, 1, 2),
    ("plain", 1, 1, 0), ("relay", 1, 1, 3), ("plain", 0, 1, 0), ("plain", 0, 0, 2),
    ("add", 0, 0, 0), ("relay", 0, 1, 1), ("relay", 1, 1, 1), ("add", 1, 0, 0),
    ("relay", 1, 1, 2), ("add", 0, 0, 1), ("plain", 1, 1, 1), ("add", 1, 0, 2),
    ("add", 0, 0, 2), ("add", 1, 1, 0), ("add", 0, 1, 0), ("add", 0, 1, 2),
    ("relay", 0, 1, 3), ("add", 1, 0, 1), ("turn", 0, 0, 0), ("plain", 0, 1, 1),
    ("plain", 1, 1, 2), ("add", 0, 1, 1), ("turn", 1, 0, 0), ("add", 1, 1, 2),
    ("add", 1, 1, 1), ("plain", 0, 1, 2), ("turn", 0, 1, 0), ("turn", 0, 0, 2),
    ("plain", 0, 0, 3), ("turn", 1, 1, 0), ("add", 0, 0, 3), ("turn", 0, 0, 1),
    ("turn", 1, 0, 1), ("add2", 0, 0), ("plain", 1, 0, 3), ("turn", 1, 0, 2),
    ("add", 1, 0, 3), ("add2", 1, 0), ("add", 0, 1, 3), ("plain", 0, 1, 3),
    ("turn", 0, 1, 1), ("turn", 1, 1, 2), ("turn", 0, 1, 2), ("add2", 0, 1),
    ("plain", 1, 1, 3), ("turn", 1, 1, 1), ("add2", 1, 1), ("add", 1, 1, 3),
    ("swap", 0, 0), ("swap", 1, 0), ("swap", 0, 1), ("swap", 1, 1),
)


def iota(shape, dim):
    return lax.broadcasted_iota(I32, shape, dim)


def encoding_rows(shape, y, z):
    row = iota(shape, 0)
    kk = row // 16
    first = (row // 4) % 4
    spot = row % 4
    second = jnp.where(spot == 0, 2, jnp.where(spot == 1, 1, jnp.where(spot == 2, 3, 0)))
    dy = jnp.where(kk == 0, first, second)
    dz = jnp.where(kk == 0, second, first)
    return 8 * ((y + dy) % 4) + 2 * ((z + dz) % 4) + kk


def kernel(
    shot_hbm, code_hbm, obs_hbm, blk_hbm, idx_hbm, wgt_hbm, out,
    xbuf, codebuf, obsbuf, blk, idx, wgt, wide, enc, inj, injc, sel,
    own, keep, send1, send2, send3, got_relay, got_turn, got_last, got_relay2, got_swap,
    load_sem, s_relay, s_turn, s_last, s_relay2, s_swap, r_relay, r_turn, r_last, r_relay2, r_swap,
):
    shot, rcv = lax.axis_index("shot"), lax.axis_index("rcv")
    y, z = shot // 4, shot % 4

    def at_shot(dy, dz):
        return (((y + dy) % 4) * 4 + (z + dz) % 4, rcv)

    def neighbour(kk, stage, direction):
        step = 1 if direction == 0 else 3
        along_y = (kk == 0) == (stage == 1)
        return at_shot(step, 0) if along_y else at_shot(0, step)

    barrier = pltpu.get_barrier_semaphore()
    for peer in (at_shot(1, 0), at_shot(3, 0), at_shot(0, 1), at_shot(0, 3)):
        pl.semaphore_signal(barrier, inc=1, device_id=peer, device_id_type=MESH)
    for off in range(1, BLOCKS):
        pl.semaphore_signal(barrier, inc=1, device_id=(shot, (rcv + off) % BLOCKS), device_id_type=MESH)

    loads = [pltpu.make_async_copy(code_hbm, codebuf, load_sem.at[0])]
    for chunk in range(4):
        rows = pl.ds(chunk * 64, 64)
        loads.append(pltpu.make_async_copy(shot_hbm.at[:, rows], xbuf.at[:, rows], load_sem.at[1 + chunk]))
    loads.append(pltpu.make_async_copy(obs_hbm, obsbuf, load_sem.at[5]))
    loads.append(pltpu.make_async_copy(blk_hbm, blk, load_sem.at[6]))
    loads.append(pltpu.make_async_copy(idx_hbm, idx, load_sem.at[7]))
    loads.append(pltpu.make_async_copy(wgt_hbm, wgt, load_sem.at[8]))
    for load in loads[:2]:
        load.start()

    pick = (encoding_rows((SUPERS, SUPERS), y, z) == iota((SUPERS, SUPERS), 1)).astype(BF16)
    widen = (iota((SHOTS_DEV, DEPTH), 1) // GROUP == iota((SHOTS_DEV, DEPTH), 0)).astype(BF16)
    same = iota((GROUP, DEPTH), 0) == iota((GROUP, DEPTH), 1) % GROUP
    loads[0].wait()
    for load in loads[2:]:
        load.start()
    codes = jnp.dot(pick, codebuf[...].astype(F32).astype(BF16), preferred_element_type=F32).astype(BF16)
    wide[...] = jnp.dot(codes, widen, preferred_element_type=F32)
    for row in range(SUPERS):
        enc[row * GROUP:(row + 1) * GROUP, :] = jnp.where(same, wide[row:row + 1, :], 0.0).astype(BF16)

    def half_rows(half):
        return pl.ds(half * HALF, HALF)

    def encode(chunk):
        half = chunk // 2
        for step in range(4):
            r0 = chunk * 64 + step * GROUP
            data = xbuf[:, r0:r0 + GROUP, :].reshape(DEPTH, SAMPLES)
            rows, inner = pl.ds(r0, GROUP), pl.ds(r0 - half * HALF, GROUP)
            for kk in range(2):
                product = jnp.dot(enc[kk * 256:(kk + 1) * 256, :], data, preferred_element_type=F32)
                product = product.reshape(4, 4, GROUP, SAMPLES)
                for th in range(2):
                    part = product[:, :, :, th * LANES:(th + 1) * LANES]
                    own[kk, th, :, rows, :] = part[0]
                    send1[kk, th, 1, :, rows, :] = part[2].astype(BF16)
                    if half == 0:
                        keep[kk, th, 0, :, inner, :] = part[1]
                        send1[kk, th, 2, :, rows, :] = part[3].astype(BF16)
                    else:
                        send1[kk, th, 0, :, rows, :] = part[1].astype(BF16)
                        keep[kk, th, 1, :, inner, :] = part[3]

    def copy1(kk, th, kind, direction, spot, part_at=None):
        unit = 2 * kk + th
        slot = 1 if kind == 0 else (0 if direction == 0 else 2)
        half = direction if kind in (0, 2) else 1 - direction
        if kind == 0:
            place, sems = got_relay.at[unit * 4 + spot, direction], (s_relay, r_relay.at[unit * 4 + spot])
        elif spot < 3:
            place, sems = got_turn.at[unit * 3 + spot, 2 * (kind - 1) + direction], (s_turn, r_turn.at[unit * 3 + spot])
        else:
            place, sems = got_last.at[unit, 2 * (kind - 1) + direction], (s_last, r_last.at[unit])
        rows = half_rows(half)
        if part_at is not None:
            rows, place = pl.ds(half * HALF + part_at * 64, 64), place.at[pl.ds(part_at * 64, 64)]
        return pltpu.make_async_remote_copy(
            src_ref=send1.at[kk, th, slot, spot, rows],
            dst_ref=place,
            send_sem=sems[0],
            recv_sem=sems[1],
            device_id=neighbour(kk, 1, direction),
            device_id_type=MESH,
        )

    def copy2(kk, th, kind, direction):
        unit = 2 * kk + th
        slot = 1 if kind == 0 else (0 if direction == 0 else 2)
        half = direction if kind in (0, 2) else 1 - direction
        if kind == 0:
            place, sems = got_relay2.at[unit, direction], (s_relay2, r_relay2.at[unit])
        else:
            place, sems = got_last.at[unit, 2 + 2 * kind + direction], (s_last, r_last.at[unit])
        return pltpu.make_async_remote_copy(
            src_ref=send2.at[kk, th, slot, half_rows(half)],
            dst_ref=place,
            send_sem=sems[0],
            recv_sem=sems[1],
            device_id=neighbour(kk, 2, direction),
            device_id_type=MESH,
        )

    def ranked(index):
        return jnp.where(index < 4, index, jnp.where(index < 6, index + 2, index - 2))

    def copy3(kk, th, off):
        block = ranked(jnp.where(off <= ranked(rcv), off - 1, off))
        return pltpu.make_async_remote_copy(
            src_ref=send3.at[kk, th, pl.ds(pl.multiple_of(block * CAP, CAP), CAP)],
            dst_ref=got_swap.at[2 * kk + th, pl.ds(pl.multiple_of(rcv * CAP, CAP), CAP)],
            send_sem=s_swap,
            recv_sem=r_swap.at[2 * kk + th],
            device_id=(shot, block),
            device_id_type=MESH,
        )

    def arrived(place, sem):
        pltpu.make_async_copy(place, place, sem).wait()

    def relay(kk, th, spot, directions=(0, 1), part_at=None):
        for direction in directions:
            copy1(kk, th, 0, direction, spot, part_at).start()

    def plain(kk, th, spot, directions=(0, 1), part_at=None):
        for direction in directions:
            copy1(kk, th, 1, direction, spot, part_at).start()

    def add(kk, th, spot):
        at = (2 * kk + th) * 4 + spot
        arrived(got_relay.at[at], r_relay.at[at])
        for direction in range(2):
            total = keep[kk, th, direction, spot] + got_relay[at, direction].astype(F32)
            send1[kk, th, 0 if direction == 0 else 2, spot, half_rows(direction), :] = total.astype(BF16)
            copy1(kk, th, 2, direction, spot).start()

    def summed(kk, th, spot, plain_at, added_at):
        return [
            own[kk, th, spot, half_rows(half), :] + added_at[half].astype(F32) + plain_at[1 - half].astype(F32)
            for half in range(2)
        ]

    def turn(kk, th, spot):
        at = (2 * kk + th) * 3 + spot
        arrived(got_turn.at[at], r_turn.at[at])
        low, high = summed(
            kk, th, spot, [got_turn[at, 0], got_turn[at, 1]], [got_turn[at, 2], got_turn[at, 3]]
        )
        if spot == 0:
            send2[kk, th, 1, half_rows(0), :] = low.astype(BF16)
            send2[kk, th, 1, half_rows(1), :] = high.astype(BF16)
            copy2(kk, th, 0, 0).start()
            copy2(kk, th, 0, 1).start()
        elif spot == 1:
            own[kk, th, 1, half_rows(0), :] = low
            send2[kk, th, 0, half_rows(1), :] = high.astype(BF16)
            copy2(kk, th, 1, 0).start()
        else:
            send2[kk, th, 2, half_rows(0), :] = low.astype(BF16)
            own[kk, th, 2, half_rows(1), :] = high
            copy2(kk, th, 1, 1).start()

    def add2(kk, th):
        unit = 2 * kk + th
        arrived(got_relay2.at[unit], r_relay2.at[unit])
        for direction in range(2):
            total = own[kk, th, 1 + direction, half_rows(direction), :] + got_relay2[unit, direction].astype(F32)
            send2[kk, th, 0 if direction == 0 else 2, half_rows(direction), :] = total.astype(BF16)
            copy2(kk, th, 2, direction).start()

    def swap(kk, th):
        unit = 2 * kk + th
        arrived(got_last.at[unit], r_last.at[unit])
        last = [got_last[unit, part] for part in range(8)]
        sums = summed(kk, th, 3, last[0:2], last[2:4])
        for half in range(2):
            total = sums[half] + last[6 + half].astype(F32) + last[5 - half].astype(F32)
            seen = obsbuf[kk, half_rows(half), th * LANES:(th + 1) * LANES].astype(F32)
            sums[half] = (total - seen).astype(BF16)
        residual = jnp.concatenate(sums, axis=0)
        packed = jnp.dot(sel[...], residual, preferred_element_type=F32).astype(BF16)
        send3[kk, th] = packed
        for off in range(1, BLOCKS):
            copy3(kk, th, off).start()
        here = pl.ds(pl.multiple_of(rcv * CAP, CAP), CAP)
        got_swap[unit, here, :] = send3[kk, th, here, :]

    def inject(kk, th):
        unit = 2 * kk + th
        arrived(got_swap.at[unit, pl.ds(0, (BLOCKS - 1) * CAP)], r_swap.at[unit])
        out[kk, :, th * LANES:(th + 1) * LANES] = jnp.dot(
            injc[...], got_swap[unit], preferred_element_type=F32
        )

    def tables():
        for load in loads[5:]:
            load.wait()
        before = (iota((RCV, RCV), 0) < iota((RCV, RCV), 1)).astype(BF16)

        def rank_of(window):
            named = (iota((BLOCKS, RCV), 0) == window).astype(F32)
            count = jnp.dot(named.astype(BF16), before, preferred_element_type=F32)
            return jnp.sum(named * count, axis=0, keepdims=True).astype(I32)

        mine = blk[:, pl.ds(pl.multiple_of(rcv * RCV, RCV), RCV)]
        sel[...] = (iota((BLOCKS * CAP, RCV), 0) == mine * CAP + rank_of(mine)).astype(BF16)
        for pair in range(BLOCKS // 2):
            chosen = []
            for side in range(2):
                start = (2 * pair + side) * RCV
                window = blk[:, start:start + RCV]
                slot = jnp.where(window == rcv, side * CAP + rank_of(window), -1)
                chosen.append((iota((2 * CAP, RCV), 0) == slot).astype(BF16))
                spread = jnp.zeros((GRID, RCV), F32)
                for which in range(STENCIL):
                    point = idx[which:which + 1, start:start + RCV]
                    weight = wgt[which:which + 1, start:start + RCV]
                    spread = spread + jnp.where(iota((GRID, RCV), 0) == point, weight, 0.0)
                inj[:, side * RCV:(side + 1) * RCV] = spread.astype(BF16)
            injc[:, pair * LANES:(pair + 1) * LANES] = lax.dot_general(
                inj[...], jnp.concatenate(chosen, axis=1), (((1,), (1,)), ((), ())), preferred_element_type=F32
            ).astype(BF16)

    for chunk in range(4):
        loads[1 + chunk].wait()
        encode(chunk)
        if chunk == 0:
            pl.semaphore_wait(barrier, 4 + BLOCKS - 1)
        for spot in range(4 if chunk < 2 else 2):
            for kk in range(2):
                relay(kk, 0, spot, (chunk // 2,), chunk % 2)
                if chunk < 2 and spot < 3:
                    plain(kk, 0, spot, (1,), chunk)
    for spot in range(2, 4):
        for kk in range(2):
            relay(kk, 0, spot, (1,))

    steps = {"relay": relay, "plain": plain, "add": add, "turn": turn, "add2": add2, "swap": swap}
    waiting = False
    for name, kk, th, *spot in SCHEDULE:
        if name not in ("relay", "plain") and not waiting:
            tables()
            waiting = True
        if name == "plain" and th == 0 and spot[0] < 3:
            plain(kk, 0, spot[0], (0,))
        else:
            steps[name](kk, th, *spot)
    for name, kk, th in [step for step in SCHEDULE if step[0] == "swap"]:
        inject(kk, th)
    arrived(got_relay, s_relay)
    arrived(got_turn, s_turn)
    arrived(got_last, s_last)
    arrived(got_relay2, s_relay2)
    arrived(got_relay.at[pl.ds(0, BLOCKS - 1)], s_swap)


def local(shot_data, code, observed, block_of, stencil_index, stencil_weight):
    dma = pltpu.SemaphoreType.DMA
    any_space = pl.BlockSpec(memory_space=pltpu.HBM)
    return pl.pallas_call(
        kernel,
        out_shape=jax.ShapeDtypeStruct((2, GRID, SAMPLES), F32),
        in_specs=[any_space] * 6,
        out_specs=pl.BlockSpec(memory_space=pltpu.VMEM),
        scratch_shapes=[
            pltpu.VMEM((SHOTS_DEV, RCV, SAMPLES), BF16),
            pltpu.VMEM((SUPERS, SHOTS_DEV), I32),
            pltpu.VMEM((2, RCV, SAMPLES), BF16),
            pltpu.VMEM((1, BLOCKS * RCV), I32),
            pltpu.VMEM((STENCIL, BLOCKS * RCV), I32),
            pltpu.VMEM((STENCIL, BLOCKS * RCV), F32),
            pltpu.VMEM((SUPERS, DEPTH), F32),
            pltpu.VMEM((ROWS, DEPTH), BF16),
            pltpu.VMEM((GRID, 2 * RCV), BF16),
            pltpu.VMEM((GRID, BLOCKS * CAP), BF16),
            pltpu.VMEM((BLOCKS * CAP, RCV), BF16),
            pltpu.VMEM((2, 2, 4, RCV, LANES), F32),
            pltpu.VMEM((2, 2, 2, 4, HALF, LANES), F32),
            pltpu.VMEM((2, 2, 3, 4, RCV, LANES), BF16),
            pltpu.VMEM((2, 2, 3, RCV, LANES), BF16),
            pltpu.VMEM((2, 2, BLOCKS * CAP, LANES), BF16),
            pltpu.VMEM((16, 2, HALF, LANES), BF16),
            pltpu.VMEM((12, 4, HALF, LANES), BF16),
            pltpu.VMEM((4, 8, HALF, LANES), BF16),
            pltpu.VMEM((4, 2, HALF, LANES), BF16),
            pltpu.VMEM((4, BLOCKS * CAP, LANES), BF16),
            dma((9,)),
            dma,
            dma,
            dma,
            dma,
            dma,
            dma((16,)),
            dma((12,)),
            dma((4,)),
            dma((4,)),
            dma((4,)),
        ],
        compiler_params=pltpu.CompilerParams(
            collective_id=0, has_side_effects=True, vmem_limit_bytes=52 * 1024 * 1024
        ),
    )(*[pltpu.with_memory_space_constraint(v, pltpu.HBM) for v in (shot_data, code, observed, block_of.T, stencil_index.T, stencil_weight.T)])


def solution(mesh):
    split = P("shot", "rcv", None)
    return jax.shard_map(
        local,
        mesh=mesh,
        in_specs=(split, P(None, "shot"), split, P(), P(), P()),
        out_specs=split,
        check_vma=False,
    )
```

```python
import jax
import jax.numpy as jnp
from jax import lax
from jax.experimental import pallas as pl
from jax.experimental.pallas import tpu as pltpu
from jax.sharding import PartitionSpec as P

SUPERS = 32
GRID = 256
STENCIL = 4
BLOCKS = 8
CAP = 64
RING = 4
RCV = 256
HALF = RCV // 2
SAMPLES = 256
LANES = 128
SHOTS_DEV = 32
GROUP = 16
ROWS = SUPERS * GROUP
DEPTH = SHOTS_DEV * GROUP
ORDER = (2, 1, 3, 0)
F32, BF16, I32 = jnp.float32, jnp.bfloat16, jnp.int32
MESH = pl.DeviceIdType.MESH
SCHEDULE = (
    ("relay", 1, 1, 0), ("plain", 0, 0, 0), ("relay", 0, 1, 0), ("plain", 0, 0, 1),
    ("plain", 1, 0, 0), ("plain", 1, 0, 1), ("plain", 1, 0, 2), ("relay", 0, 1, 2),
    ("plain", 1, 1, 0), ("relay", 1, 1, 3), ("plain", 0, 1, 0), ("plain", 0, 0, 2),
    ("add", 0, 0, 0), ("relay", 0, 1, 1), ("relay", 1, 1, 1), ("add", 1, 0, 0),
    ("relay", 1, 1, 2), ("add", 0, 0, 1), ("plain", 1, 1, 1), ("add", 1, 0, 2),
    ("add", 0, 0, 2), ("add", 1, 1, 0), ("add", 0, 1, 0), ("add", 0, 1, 2),
    ("relay", 0, 1, 3), ("add", 1, 0, 1), ("turn", 0, 0, 0), ("plain", 0, 1, 1),
    ("plain", 1, 1, 2), ("add", 0, 1, 1), ("turn", 1, 0, 0), ("add", 1, 1, 2),
    ("add", 1, 1, 1), ("plain", 0, 1, 2), ("turn", 0, 1, 0), ("turn", 0, 0, 2),
    ("plain", 0, 0, 3), ("turn", 1, 1, 0), ("add", 0, 0, 3), ("turn", 0, 0, 1),
    ("turn", 1, 0, 1), ("add2", 0, 0), ("plain", 1, 0, 3), ("turn", 1, 0, 2),
    ("add", 1, 0, 3), ("add2", 1, 0), ("add", 0, 1, 3), ("plain", 0, 1, 3),
    ("turn", 0, 1, 1), ("turn", 1, 1, 2), ("turn", 0, 1, 2), ("add2", 0, 1),
    ("plain", 1, 1, 3), ("turn", 1, 1, 1), ("add2", 1, 1), ("add", 1, 1, 3),
    ("swap", 0, 0), ("swap", 1, 0), ("swap", 0, 1), ("swap", 1, 1),
)


def iota(shape, dim):
    return lax.broadcasted_iota(I32, shape, dim)


def encoding_rows(shape, y, z):
    row = iota(shape, 0)
    kk = row // 16
    first = (row // 4) % 4
    spot = row % 4
    second = jnp.where(spot == 0, 2, jnp.where(spot == 1, 1, jnp.where(spot == 2, 3, 0)))
    dy = jnp.where(kk == 0, first, second)
    dz = jnp.where(kk == 0, second, first)
    return 8 * ((y + dy) % 4) + 2 * ((z + dz) % 4) + kk


def kernel(
    shot_hbm, code_hbm, obs_hbm, blk_hbm, idx_hbm, wgt_hbm, out,
    xbuf, codebuf, obsbuf, blk, idx, wgt, wide, enc, inj, injc, sel,
    own, keep, send1, send2, send3, got_relay, got_turn, got_last, got_relay2, got_swap,
    load_sem, s_relay, s_turn, s_last, s_relay2, s_swap, r_relay, r_turn, r_last, r_relay2, r_swap,
):
    shot, rcv = lax.axis_index("shot"), lax.axis_index("rcv")
    y, z = shot // 4, shot % 4

    def at_shot(dy, dz):
        return (((y + dy) % 4) * 4 + (z + dz) % 4, rcv)

    def neighbour(kk, stage, direction):
        step = 1 if direction == 0 else 3
        along_y = (kk == 0) == (stage == 1)
        return at_shot(step, 0) if along_y else at_shot(0, step)

    barrier = pltpu.get_barrier_semaphore()
    for peer in (at_shot(1, 0), at_shot(3, 0), at_shot(0, 1), at_shot(0, 3)):
        pl.semaphore_signal(barrier, inc=1, device_id=peer, device_id_type=MESH)
    for off in range(1, BLOCKS):
        pl.semaphore_signal(barrier, inc=1, device_id=(shot, (rcv + off) % BLOCKS), device_id_type=MESH)

    loads = [pltpu.make_async_copy(code_hbm, codebuf, load_sem.at[0])]
    for chunk in range(4):
        rows = pl.ds(chunk * 64, 64)
        loads.append(pltpu.make_async_copy(shot_hbm.at[:, rows], xbuf.at[:, rows], load_sem.at[1 + chunk]))
    loads.append(pltpu.make_async_copy(obs_hbm, obsbuf, load_sem.at[5]))
    loads.append(pltpu.make_async_copy(blk_hbm, blk, load_sem.at[6]))
    loads.append(pltpu.make_async_copy(idx_hbm, idx, load_sem.at[7]))
    loads.append(pltpu.make_async_copy(wgt_hbm, wgt, load_sem.at[8]))
    for load in loads:
        load.start()

    pick = (encoding_rows((SUPERS, SUPERS), y, z) == iota((SUPERS, SUPERS), 1)).astype(BF16)
    widen = (iota((SHOTS_DEV, DEPTH), 1) // GROUP == iota((SHOTS_DEV, DEPTH), 0)).astype(BF16)
    same = iota((GROUP, DEPTH), 0) == iota((GROUP, DEPTH), 1) % GROUP
    loads[0].wait()
    codes = jnp.dot(pick, codebuf[...].astype(F32).astype(BF16), preferred_element_type=F32).astype(BF16)
    wide[...] = jnp.dot(codes, widen, preferred_element_type=F32)
    for row in range(SUPERS):
        enc[row * GROUP:(row + 1) * GROUP, :] = jnp.where(same, wide[row:row + 1, :], 0.0).astype(BF16)

    def half_rows(half):
        return pl.ds(half * HALF, HALF)

    def encode(chunk):
        half = chunk // 2
        for step in range(4):
            r0 = chunk * 64 + step * GROUP
            data = xbuf[:, r0:r0 + GROUP, :].reshape(DEPTH, SAMPLES)
            rows, inner = pl.ds(r0, GROUP), pl.ds(r0 - half * HALF, GROUP)
            for kk in range(2):
                product = jnp.dot(enc[kk * 256:(kk + 1) * 256, :], data, preferred_element_type=F32)
                product = product.reshape(4, 4, GROUP, SAMPLES)
                for th in range(2):
                    part = product[:, :, :, th * LANES:(th + 1) * LANES]
                    own[kk, th, :, rows, :] = part[0]
                    send1[kk, th, 1, :, rows, :] = part[2].astype(BF16)
                    if half == 0:
                        keep[kk, th, 0, :, inner, :] = part[1]
                        send1[kk, th, 2, :, rows, :] = part[3].astype(BF16)
                    else:
                        send1[kk, th, 0, :, rows, :] = part[1].astype(BF16)
                        keep[kk, th, 1, :, inner, :] = part[3]

    def copy1(kk, th, kind, direction, spot, part_at=None):
        unit = 2 * kk + th
        slot = 1 if kind == 0 else (0 if direction == 0 else 2)
        half = direction if kind in (0, 2) else 1 - direction
        if kind == 0:
            place, sems = got_relay.at[unit * 4 + spot, direction], (s_relay, r_relay.at[unit * 4 + spot])
        elif spot < 3:
            place, sems = got_turn.at[unit * 3 + spot, 2 * (kind - 1) + direction], (s_turn, r_turn.at[unit * 3 + spot])
        else:
            place, sems = got_last.at[unit, 2 * (kind - 1) + direction], (s_last, r_last.at[unit])
        rows = half_rows(half)
        if part_at is not None:
            rows, place = pl.ds(half * HALF + part_at * 64, 64), place.at[pl.ds(part_at * 64, 64)]
        return pltpu.make_async_remote_copy(
            src_ref=send1.at[kk, th, slot, spot, rows],
            dst_ref=place,
            send_sem=sems[0],
            recv_sem=sems[1],
            device_id=neighbour(kk, 1, direction),
            device_id_type=MESH,
        )

    def copy2(kk, th, kind, direction):
        unit = 2 * kk + th
        slot = 1 if kind == 0 else (0 if direction == 0 else 2)
        half = direction if kind in (0, 2) else 1 - direction
        if kind == 0:
            place, sems = got_relay2.at[unit, direction], (s_relay2, r_relay2.at[unit])
        else:
            place, sems = got_last.at[unit, 2 + 2 * kind + direction], (s_last, r_last.at[unit])
        return pltpu.make_async_remote_copy(
            src_ref=send2.at[kk, th, slot, half_rows(half)],
            dst_ref=place,
            send_sem=sems[0],
            recv_sem=sems[1],
            device_id=neighbour(kk, 2, direction),
            device_id_type=MESH,
        )

    def copy3(kk, th, off):
        block = (rcv + off) % BLOCKS
        return pltpu.make_async_remote_copy(
            src_ref=send3.at[kk, th, pl.ds(off * CAP, CAP)],
            dst_ref=got_swap.at[2 * kk + th, pl.ds(pl.multiple_of(rcv * CAP, CAP), CAP)],
            send_sem=s_swap,
            recv_sem=r_swap.at[2 * kk + th],
            device_id=(shot, block),
            device_id_type=MESH,
        )

    def arrived(place, sem):
        pltpu.make_async_copy(place, place, sem).wait()

    def relay(kk, th, spot, directions=(0, 1), part_at=None):
        for direction in directions:
            copy1(kk, th, 0, direction, spot, part_at).start()

    def plain(kk, th, spot, directions=(0, 1), part_at=None):
        for direction in directions:
            copy1(kk, th, 1, direction, spot, part_at).start()

    def add(kk, th, spot):
        at = (2 * kk + th) * 4 + spot
        arrived(got_relay.at[at], r_relay.at[at])
        for direction in range(2):
            total = keep[kk, th, direction, spot] + got_relay[at, direction].astype(F32)
            send1[kk, th, 0 if direction == 0 else 2, spot, half_rows(direction), :] = total.astype(BF16)
            copy1(kk, th, 2, direction, spot).start()

    def summed(kk, th, spot, plain_at, added_at):
        return [
            own[kk, th, spot, half_rows(half), :] + added_at[half].astype(F32) + plain_at[1 - half].astype(F32)
            for half in range(2)
        ]

    def turn(kk, th, spot):
        at = (2 * kk + th) * 3 + spot
        arrived(got_turn.at[at], r_turn.at[at])
        low, high = summed(
            kk, th, spot, [got_turn[at, 0], got_turn[at, 1]], [got_turn[at, 2], got_turn[at, 3]]
        )
        if spot == 0:
            send2[kk, th, 1, half_rows(0), :] = low.astype(BF16)
            send2[kk, th, 1, half_rows(1), :] = high.astype(BF16)
            copy2(kk, th, 0, 0).start()
            copy2(kk, th, 0, 1).start()
        elif spot == 1:
            own[kk, th, 1, half_rows(0), :] = low
            send2[kk, th, 0, half_rows(1), :] = high.astype(BF16)
            copy2(kk, th, 1, 0).start()
        else:
            send2[kk, th, 2, half_rows(0), :] = low.astype(BF16)
            own[kk, th, 2, half_rows(1), :] = high
            copy2(kk, th, 1, 1).start()

    def add2(kk, th):
        unit = 2 * kk + th
        arrived(got_relay2.at[unit], r_relay2.at[unit])
        for direction in range(2):
            total = own[kk, th, 1 + direction, half_rows(direction), :] + got_relay2[unit, direction].astype(F32)
            send2[kk, th, 0 if direction == 0 else 2, half_rows(direction), :] = total.astype(BF16)
            copy2(kk, th, 2, direction).start()

    def swap(kk, th):
        unit = 2 * kk + th
        arrived(got_last.at[unit], r_last.at[unit])
        last = [got_last[unit, part] for part in range(8)]
        sums = summed(kk, th, 3, last[0:2], last[2:4])
        for half in range(2):
            total = sums[half] + last[6 + half].astype(F32) + last[5 - half].astype(F32)
            seen = obsbuf[kk, half_rows(half), th * LANES:(th + 1) * LANES].astype(F32)
            sums[half] = (total - seen).astype(BF16)
        residual = jnp.concatenate(sums, axis=0)
        for first, count in ((3, 3), (0, 3), (6, 2)):
            rows = pl.ds(first * CAP, count * CAP)
            send3[kk, th, rows, :] = jnp.dot(sel[rows, :], residual, preferred_element_type=F32).astype(BF16)
            for off in range(first, first + count):
                if off > 0:
                    copy3(kk, th, off).start()
        here = pl.ds(pl.multiple_of(rcv * CAP, CAP), CAP)
        got_swap[unit, here, :] = send3[kk, th, 0:CAP, :]

    def inject(kk, th):
        unit = 2 * kk + th
        arrived(got_swap.at[unit, pl.ds(0, (BLOCKS - 1) * CAP)], r_swap.at[unit])
        out[kk, :, th * LANES:(th + 1) * LANES] = jnp.dot(
            injc[...], got_swap[unit], preferred_element_type=F32
        )

    def tables():
        for load in loads[5:]:
            load.wait()
        before = (iota((RCV, RCV), 0) < iota((RCV, RCV), 1)).astype(BF16)

        def rank_of(window):
            named = (iota((BLOCKS, RCV), 0) == window).astype(F32)
            count = jnp.dot(named.astype(BF16), before, preferred_element_type=F32)
            return jnp.sum(named * count, axis=0, keepdims=True).astype(I32)

        mine = blk[:, pl.ds(pl.multiple_of(rcv * RCV, RCV), RCV)]
        sel[...] = (
            iota((BLOCKS * CAP, RCV), 0) == (mine - rcv + BLOCKS) % BLOCKS * CAP + rank_of(mine)
        ).astype(BF16)
        for pair in range(BLOCKS // 2):
            chosen = []
            for side in range(2):
                start = (2 * pair + side) * RCV
                window = blk[:, start:start + RCV]
                slot = jnp.where(window == rcv, side * CAP + rank_of(window), -1)
                chosen.append((iota((2 * CAP, RCV), 0) == slot).astype(BF16))
                spread = jnp.zeros((GRID, RCV), F32)
                for which in range(STENCIL):
                    point = idx[which:which + 1, start:start + RCV]
                    weight = wgt[which:which + 1, start:start + RCV]
                    spread = spread + jnp.where(iota((GRID, RCV), 0) == point, weight, 0.0)
                inj[:, side * RCV:(side + 1) * RCV] = spread.astype(BF16)
            injc[:, pair * LANES:(pair + 1) * LANES] = lax.dot_general(
                inj[...], jnp.concatenate(chosen, axis=1), (((1,), (1,)), ((), ())), preferred_element_type=F32
            ).astype(BF16)

    for chunk in range(4):
        loads[1 + chunk].wait()
        encode(chunk)
        if chunk == 0:
            pl.semaphore_wait(barrier, 4 + BLOCKS - 1)
        for spot in range(4 if chunk < 2 else 2):
            for kk in range(2):
                relay(kk, 0, spot, (chunk // 2,), chunk % 2)
                if chunk < 2 and spot < 3:
                    plain(kk, 0, spot, (1,), chunk)
    for spot in range(2, 4):
        for kk in range(2):
            relay(kk, 0, spot, (1,))

    steps = {"relay": relay, "plain": plain, "add": add, "turn": turn, "add2": add2, "swap": swap}
    waiting = False
    for name, kk, th, *spot in SCHEDULE:
        if name not in ("relay", "plain") and not waiting:
            tables()
            waiting = True
        if name == "plain" and th == 0 and spot[0] < 3:
            plain(kk, 0, spot[0], (0,))
        else:
            steps[name](kk, th, *spot)
    for name, kk, th in [step for step in SCHEDULE if step[0] == "swap"]:
        inject(kk, th)
    arrived(got_relay, s_relay)
    arrived(got_turn, s_turn)
    arrived(got_last, s_last)
    arrived(got_relay2, s_relay2)
    arrived(got_relay.at[pl.ds(0, BLOCKS - 1)], s_swap)


def local(shot_data, code, observed, block_of, stencil_index, stencil_weight):
    dma = pltpu.SemaphoreType.DMA
    any_space = pl.BlockSpec(memory_space=pltpu.HBM)
    return pl.pallas_call(
        kernel,
        out_shape=jax.ShapeDtypeStruct((2, GRID, SAMPLES), F32),
        in_specs=[any_space] * 6,
        out_specs=pl.BlockSpec(memory_space=pltpu.VMEM),
        scratch_shapes=[
            pltpu.VMEM((SHOTS_DEV, RCV, SAMPLES), BF16),
            pltpu.VMEM((SUPERS, SHOTS_DEV), I32),
            pltpu.VMEM((2, RCV, SAMPLES), BF16),
            pltpu.VMEM((1, BLOCKS * RCV), I32),
            pltpu.VMEM((STENCIL, BLOCKS * RCV), I32),
            pltpu.VMEM((STENCIL, BLOCKS * RCV), F32),
            pltpu.VMEM((SUPERS, DEPTH), F32),
            pltpu.VMEM((ROWS, DEPTH), BF16),
            pltpu.VMEM((GRID, 2 * RCV), BF16),
            pltpu.VMEM((GRID, BLOCKS * CAP), BF16),
            pltpu.VMEM((BLOCKS * CAP, RCV), BF16),
            pltpu.VMEM((2, 2, 4, RCV, LANES), F32),
            pltpu.VMEM((2, 2, 2, 4, HALF, LANES), F32),
            pltpu.VMEM((2, 2, 3, 4, RCV, LANES), BF16),
            pltpu.VMEM((2, 2, 3, RCV, LANES), BF16),
            pltpu.VMEM((2, 2, BLOCKS * CAP, LANES), BF16),
            pltpu.VMEM((16, 2, HALF, LANES), BF16),
            pltpu.VMEM((12, 4, HALF, LANES), BF16),
            pltpu.VMEM((4, 8, HALF, LANES), BF16),
            pltpu.VMEM((4, 2, HALF, LANES), BF16),
            pltpu.VMEM((4, BLOCKS * CAP, LANES), BF16),
            dma((9,)),
            dma,
            dma,
            dma,
            dma,
            dma,
            dma((16,)),
            dma((12,)),
            dma((4,)),
            dma((4,)),
            dma((4,)),
        ],
        compiler_params=pltpu.CompilerParams(
            collective_id=0, has_side_effects=True, vmem_limit_bytes=52 * 1024 * 1024
        ),
    )(*[pltpu.with_memory_space_constraint(v, pltpu.HBM) for v in (shot_data, code, observed, block_of.T, stencil_index.T, stencil_weight.T)])


def solution(mesh):
    split = P("shot", "rcv", None)
    return jax.shard_map(
        local,
        mesh=mesh,
        in_specs=(split, P(None, "shot"), split, P(), P(), P()),
        out_specs=split,
        check_vma=False,
    )
```
